256 devices in a mesh: tm: 16 (over y, x), sat: 16 (over z, core).
Axes of the slice: x: 4, y: 4, z: 8, core: 2. Of those that a mesh axis runs over, the one named last changes fastest.
Arguments:
- samples: int32 [2, 32, 8192], P(None, 'tm', 'sat'), may hold values from -1073741824 to 1073741823
- codes: int32 [48, 4092], P('sat'), may hold values from -1 to 1, as said below
- dopplers: int32 [64], replicated, may hold values from -60 to 60
Outputs:
- power: float32 [64, 48, 8192], P('tm', 'sat')
- detection: float32 [48], P('sat')
The draws below stay inside these ranges and needn't reach their ends.
Inputs may be any that keep to these rules, and one draw needn't show every extreme that they name: `codes`: each entry is -1 or 1.
All inputs are finite; a program needn't handle non-finite values.
Results may differ from the reference program's by a relative error of at most 0.0003.
Values sent between devices are 32-bit elements.
No kernel may reach another device: no remote copies, remote signals or barrier semaphores. Data moves between devices by JAX's collectives and lax.ppermute only.
A program may use at most 64 MiB of HBM per device.

```python
import math
import jax
import jax.numpy as jnp
from jax import lax

N = 8192
CHIPS = 4092
BLOCK_COUNT = 32
DOPPLER = 64
SATS = 48


def draw_samples(key, part):
    key_raw = jax.random.fold_in(key, 11)
    key_shift = jax.random.fold_in(key, 12)
    raw_words = jax.random.randint(key_raw, (2, BLOCK_COUNT, N), -1073741824, 1073741824, dtype=jnp.int32)
    shifts = jax.random.randint(key_shift, (2, BLOCK_COUNT, 32), 0, 3, dtype=jnp.int32)
    shifts = jnp.repeat(shifts, N // 32, axis=2)
    return jnp.right_shift(raw_words, shifts)


def draw_codes(key, part):
    chip_bits = jax.random.randint(jax.random.fold_in(key, 21), (SATS, CHIPS), 0, 2, dtype=jnp.int32)
    return 2 * chip_bits - 1


def with_ends(entries, stream_key, smallest, top_value):
    spot = [jax.random.randint(jax.random.fold_in(stream_key, axis), (), 0, length) for axis, length in enumerate(entries.shape)]
    main_axis = entries.shape.index(max(entries.shape))
    neighbour = spot[:main_axis] + [(spot[main_axis] + 1) % entries.shape[main_axis]] + spot[main_axis + 1:]
    return entries.at[tuple(spot)].set(smallest).at[tuple(neighbour)].set(top_value)


def setup_inputs(seed: int = 0) -> dict:
    seeds = jax.random.split(jax.random.key(seed), 4)
    return {
        "samples": draw_samples(jax.random.fold_in(seeds[3], 71), 0),
        "codes": draw_codes(jax.random.fold_in(seeds[3], 71), 0),
        "dopplers": with_ends(jax.random.randint(seeds[2], (DOPPLER,), -60, 61), jax.random.fold_in(seeds[2], 1), -60, 60).astype(jnp.int32),
    }


sample_scale = 2.0 ** -29
wrap_count = 32768


def replica_rows(codes):
    offsets = jnp.arange(N, dtype=jnp.int32)
    chip_index = (offsets * CHIPS) // N
    halves = jnp.mod((offsets * (2 * CHIPS)) // N, 2)
    sign_rows = (1 - 2 * halves).astype(jnp.float32)
    return jnp.take(codes, chip_index, axis=1).astype(jnp.float32) * sign_rows[None, :]


def reference(samples, codes, dopplers):
    real_part = samples[0].astype(jnp.float32) * sample_scale
    imag_part = samples[1].astype(jnp.float32) * sample_scale
    received_record = lax.complex(real_part, imag_part)
    spectrum = jnp.conj(jnp.fft.fft(replica_rows(codes), axis=-1))
    offsets = jnp.arange(N, dtype=jnp.int32)

    def one_bin(doppler_bin):
        rotation_angles = jnp.mod(doppler_bin * offsets, wrap_count).astype(jnp.float32) * (2.0 * math.pi / wrap_count)
        doppler_mixer = lax.complex(jnp.cos(rotation_angles), -jnp.sin(rotation_angles))
        wiped_record = jnp.fft.fft(received_record * doppler_mixer[None, :], axis=-1)

        def one_sat(code_spec):
            lagged = jnp.fft.ifft(wiped_record * code_spec[None, :], axis=-1)
            return jnp.sum(jnp.real(lagged) ** 2 + jnp.imag(lagged) ** 2, axis=0)

        return lax.map(one_sat, spectrum)

    power_map = lax.map(one_bin, dopplers) * (1.0 / (N * BLOCK_COUNT))
    average_energy = jnp.sum(real_part * real_part + imag_part * imag_part) / (BLOCK_COUNT * N)
    peak_value = jnp.max(power_map, axis=(0, 2))
    detection = peak_value / jnp.maximum(average_energy, 0.25)
    return (power_map, detection)
```

```python
import functools, math
import jax, jax.numpy as jnp, numpy as np
from jax import lax
from jax.experimental import pallas as pl
from jax.experimental.pallas import tpu as pltpu

HI, LANE = 64, 128
F32, BF16 = jnp.float32, jnp.bfloat16

def turns(num, den, sign):
    a = (num % den).astype(np.float64) * (2 * np.pi / den)
    return np.cos(a), sign * np.sin(a)

def two(x):
    hi = x.astype(jnp.bfloat16)
    return hi, (x - hi.astype(np.float64)).astype(jnp.bfloat16)

def right_matrix(sign, order=None):
    k = np.arange(LANE)
    rows = k if order is None else order
    c, s = turns(rows[:, None] * k[None, :], LANE, sign)
    hi, lo = two(np.block([[c, s], [-s, c]]))
    return np.concatenate([hi, hi, lo], axis=0)

def left_block(c, s):
    return np.block([[c, -s], [s, c]])

def left_matrix(sign):
    k = np.arange(HI)
    c, s = turns(k[:, None] * k[None, :], HI, sign)
    hi, lo = two(left_block(c, s))
    return np.concatenate([np.concatenate([hi, hi], 1), np.concatenate([lo, lo], 1)], 0)

def twist(sign, order=None):
    cols = np.arange(LANE) if order is None else order
    c, s = turns(np.arange(HI)[:, None] * cols[None, :], HI * LANE, sign)
    return np.stack([c, s]).astype(np.float32)

ORDER = np.concatenate([np.arange(0, LANE, 2), np.arange(1, LANE, 2)])

def pieces(x):
    hi = x.astype(BF16)
    return hi, (x - hi.astype(F32)).astype(BF16)

def dot(a, b):
    return jnp.dot(a, b, preferred_element_type=F32)

def joined(x_ref, i, p, b):
    low = lax.broadcasted_iota(jnp.int32, (8, 8, LANE), 1) < 4
    y, x = i // 4, i % 4
    first, second = x_ref[0, x, y, :, p], x_ref[1, x, y, :, p]
    if b == 0:
        second = pltpu.roll(second, 4, 1)
    else:
        first = pltpu.roll(first, 4, 1)
    return jnp.where(low, first, second).reshape(HI, LANE)

def main_kernel(x_ref, lf_ref, tf_ref, m_ref, c_ref, a_ref, t_ref, li_ref, out_ref, pw_ref,
                xw_ref, l_ref, y_ref, z_ref, *, nb, ns, nf):
    out_ref[...] = jnp.zeros_like(out_ref)
    R = nf * 2 * HI
    def body(i, tally):
        for b in range(2):
            for p in range(2):
                v = joined(x_ref, i, p, b).astype(F32) * (2.0 ** -29)
                tally = tally + jnp.sum((v * v).reshape(8, 8, 128), axis=0)
                hi, lo = pieces(v)
                xw_ref[p * HI:(p + 1) * HI, b * LANE:(b + 1) * LANE] = hi
                xw_ref[(2 + p) * HI:(3 + p) * HI, b * LANE:(b + 1) * LANE] = lo
        xw = xw_ref[...]
        def put(ref, row, re, im):
            for p, v in ((0, re), (1, im)):
                hi, lo = pieces(v)
                cols = slice(p * LANE, (p + 1) * LANE)
                ref[row:row + HI, p * LANE:(p + 1) * LANE] = hi
                ref[row:row + HI, 256 + p * LANE:256 + (p + 1) * LANE] = lo
        for f in range(nf):
            g = dot(lf_ref[f * 256:(f + 1) * 256], xw)
            for b in range(2):
                cols = slice(b * LANE, (b + 1) * LANE)
                zr = g[0:64, cols] + g[128:192, cols]
                zi = g[64:128, cols] + g[192:256, cols]
                tr, ti = tf_ref[f, 0], tf_ref[f, 1]
                put(l_ref, (f * 2 + b) * HI, zr * tr - zi * ti, zr * ti + zi * tr)
        spec = dot(l_ref[...], m_ref[0:512]) + dot(l_ref[:, 0:256], m_ref[512:768])
        y_ref[...] = spec
        for s in range(ns):
            cr, ci = c_ref[s, 0], c_ref[s, 1]
            for fb in range(nf * 2):
                xr = y_ref[fb * HI:(fb + 1) * HI, 0:LANE]
                xi = y_ref[fb * HI:(fb + 1) * HI, LANE:2 * LANE]
                put(l_ref, fb * HI, xr * cr + xi * ci, xi * cr - xr * ci)
            g = dot(l_ref[...], a_ref[0:512]) + dot(l_ref[:, 0:256], a_ref[512:768])
            tr, ti = t_ref[0], t_ref[1]
            for f in range(nf):
                for b in range(2):
                    rows = slice((f * 2 + b) * HI, (f * 2 + b + 1) * HI)
                    zr, zi = g[rows, 0:LANE], g[rows, LANE:2 * LANE]
                    col = slice((f * 2 + b) * LANE, (f * 2 + b + 1) * LANE)
                    for p, v in ((0, zr * tr - zi * ti), (1, zr * ti + zi * tr)):
                        hi, lo = pieces(v)
                        z_ref[p * HI:(p + 1) * HI, col] = hi
                        z_ref[(2 + p) * HI:(3 + p) * HI, col] = lo
            for f in range(0, nf, 2):
                r = dot(li_ref[...], z_ref[:, f * 256:(f + 2) * 256])
                for ff in range(2):
                    tot = None
                    for b in range(2):
                        col = slice((ff * 2 + b) * LANE, (ff * 2 + b + 1) * LANE)
                        re = r[0:64, col] + r[128:192, col]
                        im = r[64:128, col] + r[192:256, col]
                        v = re * re + im * im
                        tot = v if tot is None else tot + v
                    o = (f + ff) * ns + s
                    out_ref[o] += tot
        return tally
    tally = lax.fori_loop(0, nb // 2, body, jnp.zeros((8, 128), F32))
    pw_ref[0] = jnp.zeros((8, LANE), F32) + jnp.sum(tally)
    for s in range(ns):
        best = None
        for f in range(nf):
            v = out_ref[f * ns + s] * (2.0 ** -44)
            out_ref[f * ns + s] = v
            best = v if best is None else jnp.maximum(best, v)
        pw_ref[1 + s] = jnp.zeros((8, LANE), F32) + jnp.max(best)

def main_call(x, lf, tf, m, c, a, t, li):
    nb, ns, nf = 2 * x.shape[1] * x.shape[2], c.shape[0], tf.shape[0]
    return pl.pallas_call(
        functools.partial(main_kernel, nb=nb, ns=ns, nf=nf),
        out_shape=(jax.ShapeDtypeStruct((nf * ns, HI, LANE), F32), jax.ShapeDtypeStruct((1 + ns, 8, LANE), F32)),
        scratch_shapes=[pltpu.VMEM((256, 256), BF16), pltpu.VMEM((nf * 2 * HI, 512), BF16),
                        pltpu.VMEM((nf * 2 * HI, 256), F32), pltpu.VMEM((256, nf * 256), BF16)],
    )(x, lf, tf, m, c, a, t, li)

def code_kernel(r_ref, l_ref, t_ref, m_ref, c_ref, s_ref):
    ns = r_ref.shape[0]
    for s in range(ns):
        g = dot(l_ref[...], r_ref[s])
        zr = g[0:64] + g[128:192]
        zi = g[64:128] + g[192:256]
        tr, ti = t_ref[0], t_ref[1]
        for p, v in ((0, zr * tr - zi * ti), (1, zr * ti + zi * tr)):
            hi, lo = pieces(v)
            s_ref[s * HI:(s + 1) * HI, p * LANE:(p + 1) * LANE] = hi
            s_ref[s * HI:(s + 1) * HI, 256 + p * LANE:256 + (p + 1) * LANE] = lo
            s_ref[s * HI:(s + 1) * HI, 512 + p * LANE:512 + (p + 1) * LANE] = hi
    g = dot(s_ref[...], m_ref[...])
    for s in range(ns):
        for p in range(2):
            c_ref[s, p] = g[s * HI:(s + 1) * HI, p * LANE:(p + 1) * LANE]

def code_call(rep, l0, t0, m0):
    ns = rep.shape[0]
    return pl.pallas_call(code_kernel, out_shape=jax.ShapeDtypeStruct((ns, 2, HI, LANE), F32),
        scratch_shapes=[pltpu.VMEM((ns * HI, 768), BF16)])(rep, l0, t0, m0)

def replica(codes):
    ns = codes.shape[0]
    seg = codes.reshape(ns, 4, 1023)
    even = jnp.concatenate([seg[:, :, 0:1], seg], axis=2).reshape(ns, HI, 64)
    odd = jnp.concatenate([seg[:, :, 0:512], seg[:, :, 511:1023]], axis=2).reshape(ns, HI, 64)
    n = LANE * np.arange(HI)[:, None] + ORDER[None, :]
    sign = 1 - 2 * ((n * 8184 // 8192) % 2)
    return (jnp.concatenate([even, odd], axis=2) * jnp.asarray(sign, jnp.int32)).astype(BF16)

def code_spectra(codes):
    k = np.arange(HI)
    c, s = turns(k[:, None] * k[None, :], HI, -1.0)
    hi, lo = two(np.concatenate([c, s], 0))
    l0 = np.concatenate([hi, lo], 0)
    return code_call(replica(codes), jnp.asarray(l0), jnp.asarray(twist(-1.0, ORDER)), jnp.asarray(right_matrix(-1.0, ORDER)))

def doppler_tables(dop):
    nf = dop.shape[0]
    k = jnp.arange(HI, dtype=jnp.int32)
    num = jnp.mod(4 * k[:, None] * k[None, :] + dop[:, None, None] * k, 256).astype(F32) * (2 * math.pi / 256)
    c, s = jnp.cos(num), -jnp.sin(num)
    blk = jnp.concatenate([jnp.concatenate([c, -s], 2), jnp.concatenate([s, c], 2)], 1)
    top = lax.reduce_precision(blk, 8, 7)
    hi, lo = top.astype(BF16), (blk - top).astype(BF16)
    lf = jnp.concatenate([jnp.concatenate([hi, hi], 2), jnp.concatenate([lo, lo], 2)], 1)
    n = jnp.arange(LANE, dtype=jnp.int32)
    num = jnp.mod(4 * k[:, None] * n[None, :] + dop[:, None, None] * n, 32768).astype(F32) * (2 * math.pi / 32768)
    tf = jnp.stack([jnp.cos(num), -jnp.sin(num)], 1)
    return lf.reshape(nf * 256, 256), tf

from jax.sharding import Mesh
from jax.sharding import PartitionSpec as P

TM, SAT = ("y", "x"), ("z", "c")


def spread(x, axis):
    copies = jnp.broadcast_to(x, (lax.axis_size(axis), *x.shape))
    return lax.all_to_all(copies, axis, split_axis=0, concat_axis=0, tiled=True)


def shards(samples, codes, dopplers):
    nf = dopplers.shape[0] // lax.axis_size(TM)
    dop = lax.dynamic_slice_in_dim(dopplers, lax.axis_index(TM) * nf, nf)
    x = samples.reshape(2, 8, LANE)
    for axis in ("z", "y", "x", "c"):
        x = spread(x, axis)
    lf, tf = doppler_tables(dop)
    c = code_spectra(codes)
    power, facts = main_call(x, lf, tf, jnp.asarray(right_matrix(-1.0)), c, jnp.asarray(right_matrix(1.0)),
                             jnp.asarray(twist(1.0)), jnp.asarray(left_matrix(1.0)))
    peak = jnp.max(spread(facts[1:, 0, 0], TM), axis=0)
    mean = facts[0, 0, 0] * (1.0 / 262144)
    return power.reshape(nf, -1, HI * LANE), peak / jnp.maximum(mean, 0.25)


def solution(mesh):
    torus = Mesh(mesh.devices.reshape(4, 4, 8, 2), ("y", "x", "z", "c"))
    return jax.shard_map(
        shards, mesh=torus, in_specs=(P(None, TM, SAT), P(SAT, None), P()),
        out_specs=(P(TM, SAT, None), P(SAT)), check_vma=False,
    )
```
